32 devices in a mesh: gx: 4 (over y, x), gy: 8 (over z, core).
Axes of the slice: x: 2, y: 2, z: 4, core: 2. Of those that a mesh axis runs over, the one named last changes fastest.
Arguments:
- density: float32 [128, 256, 256], P('gx', 'gy'), may hold values from -6 to 6
- flux_east: float32 [128, 256, 256], P('gx', 'gy'), may hold values from -6 to 6
- flux_north: float32 [128, 256, 256], P('gx', 'gy'), may hold values from -6 to 6
- flux_up: float32 [128, 256, 256], P('gx', 'gy'), may hold values from -6 to 6
- theta_pert: float32 [128, 256, 256], P('gx', 'gy'), may hold values from -2 to 4
- sound_coef: bfloat16 [128, 256, 256], P('gx', 'gy'), may hold values from 0.5 to 2
- vert_inverse: float32 [512, 512], replicated, may hold values from -1 to 1
Outputs:
- density_new: float32 [128, 256, 256], P('gx', 'gy')
- east_new: float32 [128, 256, 256], P('gx', 'gy')
- north_new: float32 [128, 256, 256], P('gx', 'gy')
- upward_new: float32 [128, 256, 256], P('gx', 'gy')
- theta_new: float32 [128, 256, 256], P('gx', 'gy')
The draws below stay inside these ranges and needn't reach their ends.
All inputs are finite; a program needn't handle non-finite values.
Results may differ from the reference program's by a relative error of at most 0.0003.
Values sent between devices are 32-bit elements; how exact they have to be, the bound alone decides.
No kernel may reach another device: no remote copies, remote signals or barrier semaphores. Data moves between devices by JAX's collectives and lax.ppermute only.
A program may use at most 64 MiB of HBM per device.

```python
import math
import jax
import jax.numpy as jnp
from jax import lax

NZ = 256
SUBSTEPS = 6
NX = 128
NY = 256


def draw_theta_pert(key, part):
    return jax.random.truncated_normal(key, -2.0, 4.0, (NX, NY, NZ), jnp.float32)


def draw_vert_inverse(key, part):
    order = 2 * NZ
    spread = 0.25 / math.sqrt(order)
    offdiag = jax.random.truncated_normal(key, -4.0, 4.0, (order, order), jnp.float32) * spread
    return 0.7 * jnp.eye(order, dtype=jnp.float32) + offdiag


def shard_levels(key, dims, shards, low, high):
    loudness, own = 1.0, jax.random.fold_in(key, 6)
    for dim, shards_of in shards:
        draws = jnp.exp(jax.random.uniform(jax.random.fold_in(own, dim), (shards_of,), jnp.float32, low / len(shards), high / len(shards)))
        loudness = loudness * jnp.repeat(draws, dims[dim] // shards_of).reshape([-1 if axis == dim else 1 for axis in range(len(dims))])
    return loudness


def scatter_about(key, extent, scale, limit, cuts=(), kind=jnp.bfloat16):
    entries = jax.random.normal(key, extent, jnp.float32) * scale
    if len(cuts) > 0:
        entries = shard_levels(key, extent, cuts, -0.22, 0.18) * entries
    return jnp.clip(entries, min=-limit, max=limit).astype(kind)


def setup_inputs(seed: int = 0) -> dict:
    arg_keys = jax.random.split(jax.random.key(seed), 8)
    return {
        "density": scatter_about(arg_keys[0], (NX, NY, NZ), 1.0, 6.0, ((0, 4), (1, 8)), jnp.float32),
        "flux_east": scatter_about(arg_keys[1], (NX, NY, NZ), 1.0, 6.0, ((0, 4), (1, 8)), jnp.float32),
        "flux_north": scatter_about(arg_keys[2], (NX, NY, NZ), 1.0, 6.0, ((0, 4), (1, 8)), jnp.float32),
        "flux_up": scatter_about(arg_keys[3], (NX, NY, NZ), 1.0, 6.0, ((0, 4), (1, 8)), jnp.float32),
        "theta_pert": draw_theta_pert(jax.random.fold_in(arg_keys[7], 71), 0),
        "sound_coef": jnp.clip(jnp.exp(math.log(2.0) - 1.3862944 * jax.random.uniform(arg_keys[5], (NX, NY, NZ), jnp.float32) ** shard_levels(arg_keys[5], (NX, NY, NZ), ((0, 4), (1, 8)), -0.2, 0.2)), 0.5, 2.0).astype(jnp.bfloat16),
        "vert_inverse": draw_vert_inverse(jax.random.fold_in(arg_keys[7], 71), 0),
    }


courant = 0.45
damping = 0.1


def reference(density, flux_east, flux_north, flux_up, theta_pert, sound_coef, vert_inverse):
    coef = sound_coef.astype(jnp.float32)
    levels = density.shape[2]
    rho, east, north, upward, theta = density, flux_east, flux_north, flux_up, theta_pert
    divergence = jnp.zeros_like(density)
    for substep in range(SUBSTEPS):
        pressure = coef * theta
        east_next = east - courant * (pressure - jnp.roll(pressure, 1, 0)) + damping * (divergence - jnp.roll(divergence, 1, 0))
        north_next = north - courant * (pressure - jnp.roll(pressure, 1, 1)) + damping * (divergence - jnp.roll(divergence, 1, 1))
        level_div = (jnp.roll(east_next, -1, 0) - east_next) + (jnp.roll(north_next, -1, 1) - north_next)
        right_side = jnp.concatenate([upward, theta - courant * level_div], axis=2)
        shaped = right_side.reshape(-1, 2 * levels)
        solved = jnp.dot(shaped, vert_inverse.T, precision=lax.Precision.HIGHEST, preferred_element_type=jnp.float32)
        solved = solved.reshape(right_side.shape)
        upward = solved[:, :, :levels]
        theta = solved[:, :, levels:]
        below = jnp.concatenate([jnp.zeros_like(upward[:, :, :1]), upward[:, :, :-1]], axis=2)
        divergence = level_div + (upward - below)
        rho = rho - courant * divergence
        east, north = east_next, north_next
    return rho, east, north, upward, theta
```

```python
import jax
import jax.numpy as jnp
from jax import lax
from jax.experimental import pallas as pl
from jax.experimental.pallas import tpu as pltpu
from jax.sharding import PartitionSpec as P

SUBSTEPS = 6

courant = 0.45
damping = 0.1

MIB = 1024 * 1024
ROWS = 8
TILE = 8

ROUTES = (("gy", 1), ("gx", 1), ("gx", 0), ("gy", 0))


def paired(block, axis, odd):
    count = lax.axis_size(axis)
    route = []
    for low in range(odd, count + odd, 2):
        a, b = low % count, (low + 1) % count
        route += [(a, b), (b, a)]
    return lax.ppermute(block, axis, route)


def is_even(axis):
    return lax.axis_index(axis) % 2 == 0


def put_edges(first_x, last_x, first_y, last_y, outs):
    even_x, even_y = is_even("gx"), is_even("gy")
    outs[0][...] = jnp.where(even_y, first_y, last_y)
    outs[1][...] = jnp.where(even_x, first_x, last_x)
    outs[2][...] = jnp.where(even_x, last_x, first_x)
    outs[3][...] = jnp.where(even_y, last_y, first_y)


EVERY = slice(None)


def west_of(halo, rows=EVERY):
    return jnp.where(is_even("gx"), halo[1][rows, :], halo[2][rows, :])


def east_of(halo, rows=EVERY):
    return jnp.where(is_even("gx"), halo[2][rows, :], halo[1][rows, :])


def south_of(halo, rows=EVERY):
    return jnp.where(is_even("gy"), halo[0][rows, :], halo[3][rows, :])


def north_of(halo, rows=EVERY):
    return jnp.where(is_even("gy"), halo[3][rows, :], halo[0][rows, :])


def split(value):
    high = value.astype(jnp.bfloat16)
    low = (value - high.astype(jnp.float32)).astype(jnp.bfloat16)
    return high, low


def product(value, mat_ref):
    high, low = split(value)
    terms = jnp.concatenate([high, low, high], axis=1)
    return jnp.dot(terms, mat_ref[...], preferred_element_type=jnp.float32)


def before(rows, first):
    return jnp.concatenate([first, rows[:-1]], axis=0)


def after(rows, last):
    return jnp.concatenate([rows[1:], last], axis=0)


def level_difference(upward):
    lane = lax.broadcasted_iota(jnp.int32, upward.shape, 1)
    below = jnp.where(lane == 0, 0.0, pltpu.roll(upward, 1, 1))
    return upward - below


def first_edges_kernel(nx, ny, th_hbm, coef_hbm, u_hbm, v_hbm, *refs):
    outs, coef_out = refs[:4], refs[4]
    th_x, th_y, coef_x, coef_y, u_x, v_y, sems = refs[5:]
    copies = []

    def fetch(src, dst):
        copies.append(pltpu.make_async_copy(src, dst, sems.at[len(copies)]))
        copies[-1].start()

    for side, i in enumerate((0, nx - 1)):
        fetch(th_hbm.at[i], th_x.at[side])
        fetch(coef_hbm.at[i], coef_x.at[side])
    fetch(u_hbm.at[0], u_x)
    for side, j in enumerate((0, ny - TILE)):
        fetch(th_hbm.at[:, pl.ds(j, TILE), :], th_y.at[side])
        fetch(coef_hbm.at[:, pl.ds(j, TILE), :], coef_y.at[side])
    fetch(v_hbm.at[:, pl.ds(0, TILE), :], v_y)
    for copy in copies:
        copy.wait()
    coef = [coef_x[0].astype(jnp.float32), coef_x[1].astype(jnp.float32)]
    coef += [coef_y[side].astype(jnp.float32)[:, j, :] for side, j in enumerate((0, TILE - 1))]
    th = [th_x[0], th_x[1], th_y[0, :, 0, :], th_y[1, :, TILE - 1, :]]
    first_x, last_x, first_y, last_y = [-courant * (a * b) for a, b in zip(coef, th)]
    put_edges(u_x[...] + first_x, last_x, v_y[:, 0, :] + first_y, last_y, outs)
    coef_out[...] = jnp.concatenate(coef, axis=0)


def prepare_kernel(nx, ny, mat_ref, u_ref, v_ref, th_ref, coef_ref, h_ref, g_ref, split_ref):
    nz = u_ref.shape[1]
    order = mat_ref.shape[0]
    high, low = split(mat_ref[...].T)
    split_ref[:order] = high
    split_ref[order : 2 * order] = high
    split_ref[2 * order :] = low
    zero = jnp.zeros((1, nz), jnp.float32)
    for i in range(nx):
        here = pl.ds(i * ny, ny)
        v = v_ref[here, :]
        h = after(v, zero) - v - u_ref[here, :]
        if i + 1 < nx:
            h = h + u_ref[pl.ds((i + 1) * ny, ny), :]
        h_ref[here, :] = h
        g_ref[here, :] = -courant * (coef_ref[here, :].astype(jnp.float32) * th_ref[here, :])


def edges_kernel(nx, ny, mat_ref, coef_ref, h_ref, g_ref, w_ref, th_ref, *refs):
    halo, outs = refs[:4], refs[4:]
    nz = h_ref.shape[2]
    west, east = west_of(halo), east_of(halo)
    south, north = south_of(halo), north_of(halo)

    def plane(ref, i):
        return ref[i]

    def line(ref, j):
        return ref[:, j, :]

    def lateral(mid, lo, hi):
        return before(mid, lo) + after(mid, hi) - 4.0 * mid

    def edge(ref):
        return [plane(ref, 0), plane(ref, nx - 1), line(ref, 0), line(ref, ny - 1)]

    g, h = edge(g_ref), edge(h_ref)
    inner = [plane(g_ref, 1), plane(g_ref, nx - 2), line(g_ref, 1), line(g_ref, ny - 2)]
    lows = [south[:1], south[nx - 1 :], west[:1], west[ny - 1 :]]
    highs = [north[:1], north[nx - 1 :], east[:1], east[ny - 1 :]]
    outer = [west, east, south, north]
    level_div = jnp.concatenate(
        [
            h[s] + (inner[s] + outer[s]) + lateral(g[s], lows[s], highs[s])
            for s in range(4)
        ],
        axis=0,
    )
    theta = jnp.concatenate(edge(th_ref), axis=0) - courant * level_div
    right = jnp.concatenate([jnp.concatenate(edge(w_ref), axis=0), theta], axis=1)
    solved = product(right, mat_ref)
    div = level_div + level_difference(solved[:, :nz])
    new = damping * div - courant * (coef_ref[...] * solved[:, nz:])
    a, b, c = ny, 2 * ny, 2 * ny + nx
    put_edges(new[:a], new[a:b], new[b:c], new[c:], outs)


def around(i, nx, ny, g_ref, halo):
    mid = g_ref[pl.ds(i * ny, ny), :]
    west = west_of(halo) if i == 0 else g_ref[pl.ds((i - 1) * ny, ny), :]
    east = east_of(halo) if i == nx - 1 else g_ref[pl.ds((i + 1) * ny, ny), :]
    one = pl.ds(i, 1)
    return mid, west, east, before(mid, south_of(halo, one)), after(mid, north_of(halo, one))


def solve_planes(base, nx, ny, mat_ref, g_ref, h_ref, w_ref, th_ref, halo):
    nz = h_ref.shape[1]
    rights, divs = [], []
    for i in range(base, base + ROWS):
        here = pl.ds(i * ny, ny)
        mid, west, east, south, north = around(i, nx, ny, g_ref, halo)
        h = h_ref[here, :] + (west + east) + (south + north) - 4.0 * mid
        divs.append(h)
        rights.append(
            jnp.concatenate([w_ref[here, :], th_ref[here, :] - courant * h], axis=1)
        )
    solved = product(jnp.concatenate(rights, axis=0), mat_ref)
    for k in range(ROWS):
        q = solved[k * ny : (k + 1) * ny]
        w, th = q[:, :nz], q[:, nz:]
        here = pl.ds((base + k) * ny, ny)
        yield here, divs[k], w, th, divs[k] + level_difference(w)


def block_kernel(
    nx, ny, mat_ref, coef_ref, g_ref, h_ref, w_ref, th_ref, u_ref, v_ref, rho_ref, *refs
):
    halo = refs[:4]
    g_out, h_out, w_out, th_out, u_out, v_out, rho_out = refs[4:]
    for base in range(0, nx, ROWS):
        for i in range(base, base + ROWS):
            here = pl.ds(i * ny, ny)
            mid, west, _, south, _ = around(i, nx, ny, g_ref, halo)
            u_out[here, :] = u_ref[here, :] + (mid - west)
            v_out[here, :] = v_ref[here, :] + (mid - south)
        for here, h, w, th, div in solve_planes(
            base, nx, ny, mat_ref, g_ref, h_ref, w_ref, th_ref, halo
        ):
            h_out[here, :] = h
            rho_out[here, :] = rho_ref[here, :] - courant * div
            w_out[here, :] = w
            th_out[here, :] = th
            g_out[here, :] = damping * div - courant * (coef_ref[here, :].astype(jnp.float32) * th)


def last_kernel(nx, ny, mat_ref, g_ref, h_ref, w_ref, th_ref, u_ref, v_ref, rho_ref, *refs):
    halo, outs, parts, sems = refs[:4], refs[4:9], refs[9:14], refs[14]
    rho_part, u_part, v_part, w_part, th_part = parts
    copies = []

    def send(slot, start, count):
        rows = pl.ds(start * ny, count * ny)
        copies.append(
            pltpu.make_async_copy(
                parts[slot].at[rows, :], outs[slot].at[rows, :], sems.at[len(copies)]
            )
        )
        copies[-1].start()

    half = nx // 2
    for base in (0, half):
        for i in range(base, base + half):
            here = pl.ds(i * ny, ny)
            mid, west, _, south, _ = around(i, nx, ny, g_ref, halo)
            u_part[here, :] = u_ref[here, :] + (mid - west)
            v_part[here, :] = v_ref[here, :] + (mid - south)
        send(1, base, half)
        send(2, base, half)
    for base in range(0, nx, ROWS):
        for here, _, w, th, div in solve_planes(
            base, nx, ny, mat_ref, g_ref, h_ref, w_ref, th_ref, halo
        ):
            w_part[here, :] = w
            th_part[here, :] = th
            rho_part[here, :] = rho_ref[here, :] - courant * div
        for slot in (3, 4, 0):
            send(slot, base, ROWS)
    for copy in copies:
        copy.wait()


def body(density, flux_east, flux_north, flux_up, theta_pert, sound_coef, vert_inverse):
    nx, ny, nz = density.shape
    order = 2 * nz
    f32, bf16 = jnp.float32, jnp.bfloat16
    vmem = pl.BlockSpec(memory_space=pltpu.VMEM)
    hbm = pl.BlockSpec(memory_space=pltpu.HBM)
    plane_x = jax.ShapeDtypeStruct((ny, nz), f32)
    plane_y = jax.ShapeDtypeStruct((nx, nz), f32)
    planes = (plane_y, plane_x, plane_x, plane_y)
    field = jax.ShapeDtypeStruct((nx * ny, nz), f32)
    edge_columns = 2 * (nx + ny)

    def call(kernel, name, columns, limit=16, **options):
        return pl.pallas_call(
            lambda *refs: kernel(nx, ny, *refs),
            compiler_params=pltpu.CompilerParams(vmem_limit_bytes=limit * MIB),
            cost_estimate=pl.CostEstimate(
                flops=6 * columns * order * order,
                bytes_accessed=columns * nz * 4,
                transcendentals=0,
            ),
            name=name,
            **options,
        )

    def swapped(sends):
        return tuple(paired(block, *route) for block, route in zip(sends, ROUTES))

    *sends, coef_edges = call(
        first_edges_kernel,
        "first_edges",
        edge_columns,
        in_specs=[hbm] * 4,
        out_specs=[vmem] * 5,
        out_shape=planes + (jax.ShapeDtypeStruct((edge_columns, nz), f32),),
        scratch_shapes=[
            pltpu.VMEM((2, ny, nz), f32),
            pltpu.VMEM((2, nx, TILE, nz), f32),
            pltpu.VMEM((2, ny, nz), bf16),
            pltpu.VMEM((2, nx, TILE, nz), bf16),
            pltpu.VMEM((ny, nz), f32),
            pltpu.VMEM((nx, TILE, nz), f32),
            pltpu.SemaphoreType.DMA((10,)),
        ],
    )(
        *(
            pltpu.with_memory_space_constraint(array, pltpu.HBM)
            for array in (theta_pert, sound_coef, flux_east, flux_north)
        )
    )
    arrays = (flux_east, flux_north, flux_up, theta_pert, density, sound_coef)
    flat = tuple(array.reshape(nx * ny, nz) for array in arrays)
    sends, flat, vert_inverse = lax.optimization_barrier((sends, flat, vert_inverse))
    u, v, w, th, rho, coef = flat
    halo = swapped(sends)
    h, g, mat = call(
        prepare_kernel,
        "prepare",
        nx * ny,
        in_specs=[vmem] * 5,
        out_specs=[vmem] * 3,
        out_shape=(field, field, jax.ShapeDtypeStruct((3 * order, order), bf16)),
    )(vert_inverse, u, v, th, coef)
    for _ in range(SUBSTEPS - 1):
        sends = call(
            edges_kernel,
            "edges",
            edge_columns,
            in_specs=[vmem] * 10,
            out_specs=[vmem] * 4,
            out_shape=planes,
        )(mat, coef_edges, *(array.reshape(nx, ny, nz) for array in (h, g, w, th)), *halo)
        arrived = swapped(sends)
        g, h, w, th, u, v, rho = call(
            block_kernel,
            "block",
            nx * ny,
            in_specs=[vmem] * 13,
            out_specs=[vmem] * 7,
            out_shape=(field,) * 7,
        )(mat, coef, g, h, w, th, u, v, rho, *halo)
        halo = arrived
    outs = call(
        last_kernel,
        "last",
        nx * ny,
        limit=24,
        in_specs=[vmem] * 12,
        out_specs=[hbm] * 5,
        out_shape=(field,) * 5,
        scratch_shapes=[pltpu.VMEM((nx * ny, nz), f32)] * 5
        + [pltpu.SemaphoreType.DMA((4 + 3 * (nx // ROWS),))],
    )(mat, g, h, w, th, u, v, rho, *halo)
    return tuple(out.reshape(nx, ny, nz) for out in outs)


def solution(mesh):
    spec = P("gx", "gy", None)
    return jax.shard_map(
        body, mesh=mesh, in_specs=(spec,) * 6 + (P(),), out_specs=(spec,) * 5, check_vma=False
    )
```

```python
import functools

import jax
import jax.numpy as jnp
from jax import lax
from jax.experimental import pallas as pl
from jax.experimental.pallas import tpu as pltpu
from jax.sharding import PartitionSpec as P

SUBSTEPS = 6

courant = 0.45
damping = 0.1

MIB = 1024 * 1024
ROWS = 8
TILE = 8

ROUTES = (("gy", 1), ("gx", 1), ("gx", 0), ("gy", 0))


def paired(block, axis, odd):
    count = lax.axis_size(axis)
    route = []
    for low in range(odd, count + odd, 2):
        a, b = low % count, (low + 1) % count
        route += [(a, b), (b, a)]
    return lax.ppermute(block, axis, route)


def is_even(axis):
    return lax.axis_index(axis) % 2 == 0


def put_edges(first_x, last_x, first_y, last_y, outs):
    even_x, even_y = is_even("gx"), is_even("gy")
    outs[0][...] = jnp.where(even_y, first_y, last_y)
    outs[1][...] = jnp.where(even_x, first_x, last_x)
    outs[2][...] = jnp.where(even_x, last_x, first_x)
    outs[3][...] = jnp.where(even_y, last_y, first_y)


EVERY = slice(None)


def west_of(halo, rows=EVERY):
    return jnp.where(is_even("gx"), halo[1][rows, :], halo[2][rows, :])


def east_of(halo, rows=EVERY):
    return jnp.where(is_even("gx"), halo[2][rows, :], halo[1][rows, :])


def south_of(halo, rows=EVERY):
    return jnp.where(is_even("gy"), halo[0][rows, :], halo[3][rows, :])


def north_of(halo, rows=EVERY):
    return jnp.where(is_even("gy"), halo[3][rows, :], halo[0][rows, :])


def split(value):
    high = value.astype(jnp.bfloat16)
    low = (value - high.astype(jnp.float32)).astype(jnp.bfloat16)
    return high, low


def product(upward, theta, mat_ref):
    terms = []
    for value in (upward, theta):
        high, low = split(value)
        terms += [high, low, high]
    terms = jnp.concatenate(terms, axis=1)
    return jnp.dot(terms, mat_ref[...], preferred_element_type=jnp.float32)


def before(rows, first):
    return jnp.concatenate([first, rows[:-1]], axis=0)


def after(rows, last):
    return jnp.concatenate([rows[1:], last], axis=0)


def level_difference(upward):
    lane = lax.broadcasted_iota(jnp.int32, upward.shape, 1)
    below = jnp.where(lane == 0, 0.0, pltpu.roll(upward, 1, 1))
    return upward - below


def first_edges_kernel(nx, ny, th_hbm, coef_hbm, u_hbm, v_hbm, *refs):
    outs, coef_out = refs[:4], refs[4]
    th_x, th_y, coef_x, coef_y, u_x, v_y, sems = refs[5:]
    copies = []

    def fetch(src, dst):
        copies.append(pltpu.make_async_copy(src, dst, sems.at[len(copies)]))
        copies[-1].start()

    for side, i in enumerate((0, nx - 1)):
        fetch(th_hbm.at[i], th_x.at[side])
        fetch(coef_hbm.at[i], coef_x.at[side])
    fetch(u_hbm.at[0], u_x)
    for side, j in enumerate((0, ny - TILE)):
        fetch(coef_hbm.at[:, pl.ds(j, TILE), :], coef_y.at[side])
    for side, j in enumerate((0, ny - 1)):
        fetch(th_hbm.at[:, j, :], th_y.at[side])
    fetch(v_hbm.at[:, 0, :], v_y)
    for copy in copies:
        copy.wait()
    coef = [coef_x[0].astype(jnp.float32), coef_x[1].astype(jnp.float32)]
    coef += [coef_y[side].astype(jnp.float32)[:, j, :] for side, j in enumerate((0, TILE - 1))]
    th = [th_x[0], th_x[1], th_y[0], th_y[1]]
    first_x, last_x, first_y, last_y = [-courant * (a * b) for a, b in zip(coef, th)]
    put_edges(u_x[...] + first_x, last_x, v_y[...] + first_y, last_y, outs)
    coef_out[...] = jnp.concatenate(coef, axis=0)


def prepare_kernel(nx, ny, mat_hbm, u_hbm, v_hbm, th_hbm, coef_hbm, *refs):
    h_ref, g_ref, split_ref, u_ref, v_ref, th_ref, coef_ref, mat_ref, sems = refs
    nz = u_ref.shape[1]
    order = mat_ref.shape[0]
    pairs = (
        (mat_hbm, mat_ref),
        (v_hbm, v_ref),
        (u_hbm, u_ref),
        (coef_hbm, coef_ref),
        (th_hbm, th_ref),
    )
    copies = [pltpu.make_async_copy(*pair, sems.at[k]) for k, pair in enumerate(pairs)]
    for copy in copies:
        copy.start()
    copies[0].wait()
    high, low = split(mat_ref[...].T)
    for part in range(2):
        rows = slice(part * nz, (part + 1) * nz)
        for slot, factor in enumerate((high, high, low)):
            split_ref[pl.ds((3 * part + slot) * nz, nz), :] = factor[rows]
    copies[1].wait()
    copies[2].wait()
    zero = jnp.zeros((1, nz), jnp.float32)
    for i in range(nx):
        here = pl.ds(i * ny, ny)
        v = v_ref[here, :]
        h = after(v, zero) - v - u_ref[here, :]
        if i + 1 < nx:
            h = h + u_ref[pl.ds((i + 1) * ny, ny), :]
        h_ref[here, :] = h
    copies[3].wait()
    copies[4].wait()
    for i in range(nx):
        here = pl.ds(i * ny, ny)
        g_ref[here, :] = -courant * (coef_ref[here, :].astype(jnp.float32) * th_ref[here, :])


def edges_kernel(packed, nx, ny, mat_ref, coef_ref, h_ref, w_ref, th_ref, edge_g_ref, g_ref, *refs):
    halo, outs = refs[:4], refs[4:8]
    nz = g_ref.shape[2]
    west, east = west_of(halo), east_of(halo)
    south, north = south_of(halo), north_of(halo)
    a, b, c, d = ny, 2 * ny, 2 * ny + nx, 2 * (ny + nx)
    bounds = ((0, a), (a, b), (b, c), (c, d))

    def plane(ref, i):
        return ref[i]

    def line(ref, j):
        return ref[:, j, :]

    def lateral(mid, lo, hi):
        return before(mid, lo) + after(mid, hi) - 4.0 * mid

    def edge(ref):
        if packed:
            return ref[...]
        parts = [plane(ref, 0), plane(ref, nx - 1), line(ref, 0), line(ref, ny - 1)]
        return jnp.concatenate(parts, axis=0)

    g = edge(edge_g_ref)
    inner = [plane(g_ref, 1), plane(g_ref, nx - 2), line(g_ref, 1), line(g_ref, ny - 2)]
    lows = [south[:1], south[nx - 1 :], west[:1], west[ny - 1 :]]
    highs = [north[:1], north[nx - 1 :], east[:1], east[ny - 1 :]]
    outer = [west, east, south, north]
    change = [
        (inner[s] + outer[s]) + lateral(g[slice(*bounds[s])], lows[s], highs[s]) for s in range(4)
    ]
    level_div = edge(h_ref) + jnp.concatenate(change, axis=0)
    theta = edge(th_ref) - courant * level_div
    solved = product(edge(w_ref), theta, mat_ref)
    upward, theta = solved[:, :nz], solved[:, nz:]
    div = level_div + level_difference(upward)
    new = damping * div - courant * (coef_ref[...] * theta)
    put_edges(*(new[slice(*bound)] for bound in bounds), outs)
    for ref, value in zip(refs[8:], (level_div, upward, theta, new)):
        ref[...] = value


def around(i, nx, ny, g_ref, halo):
    mid = g_ref[pl.ds(i * ny, ny), :]
    west = west_of(halo) if i == 0 else g_ref[pl.ds((i - 1) * ny, ny), :]
    east = east_of(halo) if i == nx - 1 else g_ref[pl.ds((i + 1) * ny, ny), :]
    one = pl.ds(i, 1)
    return mid, west, east, before(mid, south_of(halo, one)), after(mid, north_of(halo, one))


def solve_planes(base, count, nx, ny, mat_ref, g_ref, h_ref, w_ref, th_ref, halo):
    nz = h_ref.shape[1]
    ws, ths, divs = [], [], []
    for i in range(base, base + count):
        here = pl.ds(i * ny, ny)
        mid, west, east, south, north = around(i, nx, ny, g_ref, halo)
        h = h_ref[here, :] + (west + east) + (south + north) - 4.0 * mid
        divs.append(h)
        ws.append(w_ref[here, :])
        ths.append(th_ref[here, :] - courant * h)
    solved = product(jnp.concatenate(ws, axis=0), jnp.concatenate(ths, axis=0), mat_ref)
    for k in range(count):
        q = solved[k * ny : (k + 1) * ny]
        w, th = q[:, :nz], q[:, nz:]
        here = pl.ds((base + k) * ny, ny)
        yield here, divs[k], w, th, divs[k] + level_difference(w)


def block_kernel(
    nx, ny, mat_ref, coef_ref, g_ref, h_ref, w_ref, th_ref, u_ref, v_ref, rho_ref, *refs
):
    halo = refs[:4]
    g_out, h_out, w_out, th_out, u_out, v_out, rho_out = refs[4:]
    for base in range(0, nx, ROWS):
        for i in range(base, base + ROWS):
            here = pl.ds(i * ny, ny)
            mid, west, _, south, _ = around(i, nx, ny, g_ref, halo)
            u_out[here, :] = u_ref[here, :] + (mid - west)
            v_out[here, :] = v_ref[here, :] + (mid - south)
        for here, h, w, th, div in solve_planes(
            base, ROWS, nx, ny, mat_ref, g_ref, h_ref, w_ref, th_ref, halo
        ):
            h_out[here, :] = h
            rho_out[here, :] = rho_ref[here, :] - courant * div
            w_out[here, :] = w
            th_out[here, :] = th
            g_out[here, :] = damping * div - courant * (coef_ref[here, :].astype(jnp.float32) * th)


def last_pieces(nx):
    pieces = [(base, ROWS) for base in range(0, nx - ROWS, ROWS)]
    half = ROWS // 2
    return pieces + [(nx - ROWS, half), (nx - half, half)]


def last_kernel(nx, ny, mat_ref, g_ref, h_ref, w_ref, th_ref, u_ref, v_ref, rho_ref, *refs):
    halo, outs, parts, sems = refs[:4], refs[4:9], refs[9:14], refs[14]
    rho_part, u_part, v_part, w_part, th_part = parts
    copies = []

    def send(slot, start, count):
        rows = pl.ds(start * ny, count * ny)
        copies.append(
            pltpu.make_async_copy(
                parts[slot].at[rows, :], outs[slot].at[rows, :], sems.at[len(copies)]
            )
        )
        copies[-1].start()

    def fluxes(base, count):
        for i in range(base, base + count):
            here = pl.ds(i * ny, ny)
            mid, west, _, south, _ = around(i, nx, ny, g_ref, halo)
            u_part[here, :] = u_ref[here, :] + (mid - west)
            v_part[here, :] = v_ref[here, :] + (mid - south)
        for slot in (1, 2):
            send(slot, base, count)

    pieces = last_pieces(nx)
    for base, count in pieces:
        if base == 0:
            fluxes(base, count)
        if base + count < nx:
            ahead = dict(pieces)[base + count]
            fluxes(base + count, ahead)
        for here, _, w, th, div in solve_planes(
            base, count, nx, ny, mat_ref, g_ref, h_ref, w_ref, th_ref, halo
        ):
            w_part[here, :] = w
            th_part[here, :] = th
            rho_part[here, :] = rho_ref[here, :] - courant * div
        for slot in (3, 4, 0):
            send(slot, base, count)
    for copy in copies:
        copy.wait()


def body(density, flux_east, flux_north, flux_up, theta_pert, sound_coef, vert_inverse):
    nx, ny, nz = density.shape
    order = 2 * nz
    f32, bf16 = jnp.float32, jnp.bfloat16
    vmem = pl.BlockSpec(memory_space=pltpu.VMEM)
    hbm = pl.BlockSpec(memory_space=pltpu.HBM)
    plane_x = jax.ShapeDtypeStruct((ny, nz), f32)
    plane_y = jax.ShapeDtypeStruct((nx, nz), f32)
    planes = (plane_y, plane_x, plane_x, plane_y)
    field = jax.ShapeDtypeStruct((nx * ny, nz), f32)
    edge_columns = 2 * (nx + ny)

    def call(kernel, name, columns, limit=16, **options):
        return pl.pallas_call(
            lambda *refs: kernel(nx, ny, *refs),
            compiler_params=pltpu.CompilerParams(vmem_limit_bytes=limit * MIB),
            cost_estimate=pl.CostEstimate(
                flops=6 * columns * order * order,
                bytes_accessed=columns * nz * 4,
                transcendentals=0,
            ),
            name=name,
            **options,
        )

    def swapped(sends):
        return tuple(paired(block, *route) for block, route in zip(sends, ROUTES))

    *sends, coef_edges = call(
        first_edges_kernel,
        "first_edges",
        edge_columns,
        in_specs=[hbm] * 4,
        out_specs=[vmem] * 5,
        out_shape=planes + (jax.ShapeDtypeStruct((edge_columns, nz), f32),),
        scratch_shapes=[
            pltpu.VMEM((2, ny, nz), f32),
            pltpu.VMEM((2, nx, nz), f32),
            pltpu.VMEM((2, ny, nz), bf16),
            pltpu.VMEM((2, nx, TILE, nz), bf16),
            pltpu.VMEM((ny, nz), f32),
            pltpu.VMEM((nx, nz), f32),
            pltpu.SemaphoreType.DMA((10,)),
        ],
    )(
        *(
            pltpu.with_memory_space_constraint(array, pltpu.HBM)
            for array in (theta_pert, sound_coef, flux_east, flux_north)
        )
    )
    arrays = (flux_east, flux_north, flux_up, theta_pert, density, sound_coef)
    flat = tuple(array.reshape(nx * ny, nz) for array in arrays)
    sends, flat, vert_inverse = lax.optimization_barrier((sends, flat, vert_inverse))
    u, v, w, th, rho, coef = flat
    halo = swapped(sends)
    h, g, mat, u, v, th, coef = call(
        prepare_kernel,
        "prepare",
        nx * ny,
        in_specs=[hbm] * 5,
        out_specs=[vmem] * 7,
        out_shape=(field, field, jax.ShapeDtypeStruct((3 * order, order), bf16))
        + (field,) * 3
        + (jax.ShapeDtypeStruct((nx * ny, nz), bf16),),
        scratch_shapes=[pltpu.VMEM((order, order), f32), pltpu.SemaphoreType.DMA((5,))],
    )(*(pltpu.with_memory_space_constraint(x, pltpu.HBM) for x in (vert_inverse, u, v, th, coef)))
    edge_state = tuple(array.reshape(nx, ny, nz) for array in (h, w, th, g))
    for substep in range(SUBSTEPS - 1):
        kept = 4 if substep < SUBSTEPS - 2 else 0
        new_state = call(
            functools.partial(edges_kernel, substep > 0),
            "edges",
            edge_columns,
            in_specs=[vmem] * 11,
            out_specs=[vmem] * (4 + kept),
            out_shape=planes + (jax.ShapeDtypeStruct((edge_columns, nz), f32),) * kept,
        )(mat, coef_edges, *edge_state, g.reshape(nx, ny, nz), *halo)
        sends, edge_state = new_state[:4], new_state[4:]
        arrived = swapped(sends)
        g, h, w, th, u, v, rho = call(
            block_kernel,
            "block",
            nx * ny,
            in_specs=[vmem] * 13,
            out_specs=[vmem] * 7,
            out_shape=(field,) * 7,
        )(mat, coef, g, h, w, th, u, v, rho, *halo)
        halo = arrived
    outs = call(
        last_kernel,
        "last",
        nx * ny,
        limit=24,
        in_specs=[vmem] * 12,
        out_specs=[hbm] * 5,
        out_shape=(field,) * 5,
        scratch_shapes=[pltpu.VMEM((nx * ny, nz), f32)] * 5
        + [pltpu.SemaphoreType.DMA((5 * len(last_pieces(nx)),))],
    )(mat, g, h, w, th, u, v, rho, *halo)
    return tuple(out.reshape(nx, ny, nz) for out in outs)


def solution(mesh):
    spec = P("gx", "gy", None)
    return jax.shard_map(
        body, mesh=mesh, in_specs=(spec,) * 6 + (P(),), out_specs=(spec,) * 5, check_vma=False
    )
```

```python
import functools

import jax
import jax.numpy as jnp
from jax import lax
from jax.experimental import pallas as pl
from jax.experimental.pallas import tpu as pltpu
from jax.sharding import PartitionSpec as P

SUBSTEPS = 6

courant = 0.45
damping = 0.1

MIB = 1024 * 1024
ROWS = 8
LAST_ROWS = 4
FLUX_ROWS = 8
TILE = 8

ROUTES = (("gy", 1), ("gx", 1), ("gx", 0), ("gy", 0))


def paired(block, axis, odd):
    count = lax.axis_size(axis)
    route = []
    for low in range(odd, count + odd, 2):
        a, b = low % count, (low + 1) % count
        route += [(a, b), (b, a)]
    return lax.ppermute(block, axis, route)


def is_even(axis):
    return lax.axis_index(axis) % 2 == 0


def put_edges(first_x, last_x, first_y, last_y, outs):
    even_x, even_y = is_even("gx"), is_even("gy")
    outs[0][...] = jnp.where(even_y, first_y, last_y)
    outs[1][...] = jnp.where(even_x, first_x, last_x)
    outs[2][...] = jnp.where(even_x, last_x, first_x)
    outs[3][...] = jnp.where(even_y, last_y, first_y)


EVERY = slice(None)


def west_of(halo, rows=EVERY):
    return jnp.where(is_even("gx"), halo[1][rows, :], halo[2][rows, :])


def east_of(halo, rows=EVERY):
    return jnp.where(is_even("gx"), halo[2][rows, :], halo[1][rows, :])


def south_of(halo, rows=EVERY):
    return jnp.where(is_even("gy"), halo[0][rows, :], halo[3][rows, :])


def north_of(halo, rows=EVERY):
    return jnp.where(is_even("gy"), halo[3][rows, :], halo[0][rows, :])


def split(value):
    high = value.astype(jnp.bfloat16)
    low = (value - high.astype(jnp.float32)).astype(jnp.bfloat16)
    return high, low


def product(upward, theta, mat_ref):
    terms = []
    for value in (upward, theta):
        high, low = split(value)
        terms += [high, low, high]
    terms = jnp.concatenate(terms, axis=1)
    return jnp.dot(terms, mat_ref[...], preferred_element_type=jnp.float32)


def before(rows, first):
    return jnp.concatenate([first, rows[:-1]], axis=0)


def after(rows, last):
    return jnp.concatenate([rows[1:], last], axis=0)


def level_difference(upward):
    lane = lax.broadcasted_iota(jnp.int32, upward.shape, 1)
    below = jnp.where(lane == 0, 0.0, pltpu.roll(upward, 1, 1))
    return upward - below


def first_edges_kernel(nx, ny, th_hbm, coef_hbm, u_hbm, v_hbm, *refs):
    outs, coef_out = refs[:4], refs[4]
    th_x, th_y, coef_x, coef_y, u_x, v_y, sems = refs[5:]
    copies = []

    def fetch(src, dst):
        copies.append(pltpu.make_async_copy(src, dst, sems.at[len(copies)]))
        copies[-1].start()

    for side, i in enumerate((0, nx - 1)):
        fetch(th_hbm.at[i], th_x.at[side])
        fetch(coef_hbm.at[i], coef_x.at[side])
    fetch(u_hbm.at[0], u_x)
    for side, j in enumerate((0, ny - TILE)):
        fetch(coef_hbm.at[:, pl.ds(j, TILE), :], coef_y.at[side])
    for side, j in enumerate((0, ny - 1)):
        fetch(th_hbm.at[:, j, :], th_y.at[side])
    fetch(v_hbm.at[:, 0, :], v_y)
    for copy in copies:
        copy.wait()
    coef = [coef_x[0].astype(jnp.float32), coef_x[1].astype(jnp.float32)]
    coef += [coef_y[side].astype(jnp.float32)[:, j, :] for side, j in enumerate((0, TILE - 1))]
    th = [th_x[0], th_x[1], th_y[0], th_y[1]]
    first_x, last_x, first_y, last_y = [-courant * (a * b) for a, b in zip(coef, th)]
    put_edges(u_x[...] + first_x, last_x, v_y[...] + first_y, last_y, outs)
    coef_out[...] = jnp.concatenate(coef, axis=0)


def prepare_kernel(nx, ny, mat_hbm, u_hbm, v_hbm, th_hbm, coef_hbm, *refs):
    h_ref, g_ref, split_ref, u_ref, v_ref, th_ref, coef_ref, mat_ref, sems = refs
    nz = u_ref.shape[1]
    order = mat_ref.shape[0]
    pairs = (
        (mat_hbm, mat_ref),
        (v_hbm, v_ref),
        (u_hbm, u_ref),
        (coef_hbm, coef_ref),
        (th_hbm, th_ref),
    )
    copies = [pltpu.make_async_copy(*pair, sems.at[k]) for k, pair in enumerate(pairs)]
    for copy in copies:
        copy.start()
    copies[0].wait()
    high, low = split(mat_ref[...].T)
    for part in range(2):
        rows = slice(part * nz, (part + 1) * nz)
        for slot, factor in enumerate((high, high, low)):
            split_ref[pl.ds((3 * part + slot) * nz, nz), :] = factor[rows]
    copies[1].wait()
    copies[2].wait()
    zero = jnp.zeros((1, nz), jnp.float32)
    for i in range(nx):
        here = pl.ds(i * ny, ny)
        v = v_ref[here, :]
        h = after(v, zero) - v - u_ref[here, :]
        if i + 1 < nx:
            h = h + u_ref[pl.ds((i + 1) * ny, ny), :]
        h_ref[here, :] = h
    copies[3].wait()
    copies[4].wait()
    for i in range(nx):
        here = pl.ds(i * ny, ny)
        g_ref[here, :] = -courant * (coef_ref[here, :].astype(jnp.float32) * th_ref[here, :])


def edges_kernel(packed, nx, ny, mat_ref, coef_ref, h_ref, w_ref, th_ref, edge_g_ref, g_ref, *refs):
    halo, outs = refs[:4], refs[4:8]
    nz = g_ref.shape[2]
    west, east = west_of(halo), east_of(halo)
    south, north = south_of(halo), north_of(halo)
    a, b, c, d = ny, 2 * ny, 2 * ny + nx, 2 * (ny + nx)
    bounds = ((0, a), (a, b), (b, c), (c, d))

    def plane(ref, i):
        return ref[i]

    def line(ref, j):
        return ref[:, j, :]

    def lateral(mid, lo, hi):
        return before(mid, lo) + after(mid, hi) - 4.0 * mid

    def edge(ref):
        if packed:
            return ref[...]
        parts = [plane(ref, 0), plane(ref, nx - 1), line(ref, 0), line(ref, ny - 1)]
        return jnp.concatenate(parts, axis=0)

    g = edge(edge_g_ref)
    inner = [plane(g_ref, 1), plane(g_ref, nx - 2), line(g_ref, 1), line(g_ref, ny - 2)]
    lows = [south[:1], south[nx - 1 :], west[:1], west[ny - 1 :]]
    highs = [north[:1], north[nx - 1 :], east[:1], east[ny - 1 :]]
    outer = [west, east, south, north]
    change = [
        (inner[s] + outer[s]) + lateral(g[slice(*bounds[s])], lows[s], highs[s]) for s in range(4)
    ]
    level_div = edge(h_ref) + jnp.concatenate(change, axis=0)
    theta = edge(th_ref) - courant * level_div
    solved = product(edge(w_ref), theta, mat_ref)
    upward, theta = solved[:, :nz], solved[:, nz:]
    div = level_div + level_difference(upward)
    new = damping * div - courant * (coef_ref[...] * theta)
    put_edges(*(new[slice(*bound)] for bound in bounds), outs)
    for ref, value in zip(refs[8:], (level_div, upward, theta, new)):
        ref[...] = value


def around(i, nx, ny, g_ref, halo):
    mid = g_ref[pl.ds(i * ny, ny), :]
    west = west_of(halo) if i == 0 else g_ref[pl.ds((i - 1) * ny, ny), :]
    east = east_of(halo) if i == nx - 1 else g_ref[pl.ds((i + 1) * ny, ny), :]
    one = pl.ds(i, 1)
    return mid, west, east, before(mid, south_of(halo, one)), after(mid, north_of(halo, one))


def solve_planes(base, count, nx, ny, mat_ref, g_ref, h_ref, w_ref, th_ref, halo, h_out):
    nz = h_ref.shape[1]
    ws, ths = [], []
    for i in range(base, base + count):
        here = pl.ds(i * ny, ny)
        mid, west, east, south, north = around(i, nx, ny, g_ref, halo)
        h = h_ref[here, :] + (west + east) + (south + north) - 4.0 * mid
        h_out[here, :] = h
        ws.append(w_ref[here, :])
        ths.append(th_ref[here, :] - courant * h)
    solved = product(jnp.concatenate(ws, axis=0), jnp.concatenate(ths, axis=0), mat_ref)
    for k in range(count):
        q = solved[k * ny : (k + 1) * ny]
        w, th = q[:, :nz], q[:, nz:]
        here = pl.ds((base + k) * ny, ny)
        yield here, w, th, h_out[here, :] + level_difference(w)


def block_kernel(
    nx, ny, mat_ref, coef_ref, g_ref, h_ref, w_ref, th_ref, u_ref, v_ref, rho_ref, *refs
):
    edge_h, edge_w, edge_th, edge_g = refs[:4]
    halo = refs[4:8]
    g_out, h_out, w_out, th_out, u_out, v_out, rho_out = refs[8:]

    def fluxes(planes):
        for i in planes:
            here = pl.ds(i * ny, ny)
            mid, west, _, south, _ = around(i, nx, ny, g_ref, halo)
            u_out[here, :] = u_ref[here, :] + (mid - west)
            v_out[here, :] = v_ref[here, :] + (mid - south)

    for side, i in enumerate((0, nx - 1)):
        here, there = pl.ds(i * ny, ny), pl.ds(side * ny, ny)
        h, w = edge_h[there, :], edge_w[there, :]
        h_out[here, :] = h
        w_out[here, :] = w
        th_out[here, :] = edge_th[there, :]
        g_out[here, :] = edge_g[there, :]
        rho_out[here, :] = rho_ref[here, :] - courant * (h + level_difference(w))
    fluxes((0, nx - 1))
    for base in range(1, nx - 1, ROWS):
        count = min(ROWS, nx - 1 - base)
        fluxes(range(base, base + count))
        for here, w, th, div in solve_planes(
            base, count, nx, ny, mat_ref, g_ref, h_ref, w_ref, th_ref, halo, h_out
        ):
            rho_out[here, :] = rho_ref[here, :] - courant * div
            w_out[here, :] = w
            th_out[here, :] = th
            g_out[here, :] = damping * div - courant * (coef_ref[here, :].astype(jnp.float32) * th)


def last_kernel(nx, ny, mat_ref, g_ref, h_ref, w_ref, th_ref, u_ref, v_ref, rho_ref, *refs):
    halo, outs, parts = refs[:4], refs[4:9], refs[9:14]
    sems, flux_sems = refs[14:]
    rho_part, u_part, v_part, w_part, th_part = parts
    copies = []

    def flux_copy(slot, rows, sem):
        return pltpu.make_async_copy(
            parts[slot].at[rows, :], outs[slot].at[rows, :], flux_sems.at[sem]
        )

    def send(slot, start, count):
        rows = pl.ds(start * ny, count * ny)
        copies.append(
            pltpu.make_async_copy(
                parts[slot].at[rows, :], outs[slot].at[rows, :], sems.at[len(copies)]
            )
        )
        copies[-1].start()

    @pl.loop(0, nx // FLUX_ROWS)
    def fluxes(step):
        base = step * FLUX_ROWS
        for k in range(FLUX_ROWS):
            i = base + k
            here = pl.ds(pl.multiple_of(i * ny, ny), ny)
            mid = g_ref[here, :]
            back = jnp.maximum(i - 1, 0) if k == 0 else i - 1
            west = g_ref[pl.ds(pl.multiple_of(back * ny, ny), ny), :]
            if k == 0:
                west = jnp.where(base == 0, west_of(halo), west)
            south = before(mid, south_of(halo, pl.ds(i, 1)))
            u_part[here, :] = u_ref[here, :] + (mid - west)
            v_part[here, :] = v_ref[here, :] + (mid - south)
        rows = pl.ds(pl.multiple_of(base * ny, FLUX_ROWS * ny), FLUX_ROWS * ny)
        for slot in (1, 2):
            flux_copy(slot, rows, 2 * step + slot - 1).start()

    for base in range(0, nx, LAST_ROWS):
        for here, w, th, div in solve_planes(
            base, LAST_ROWS, nx, ny, mat_ref, g_ref, h_ref, w_ref, th_ref, halo, rho_part
        ):
            w_part[here, :] = w
            th_part[here, :] = th
            rho_part[here, :] = rho_ref[here, :] - courant * div
        for slot in (3, 4, 0):
            send(slot, base, LAST_ROWS)
    for step in range(nx // FLUX_ROWS):
        rows = pl.ds(step * FLUX_ROWS * ny, FLUX_ROWS * ny)
        for slot in (1, 2):
            flux_copy(slot, rows, 2 * step + slot - 1).wait()
    for copy in copies:
        copy.wait()


def body(density, flux_east, flux_north, flux_up, theta_pert, sound_coef, vert_inverse):
    nx, ny, nz = density.shape
    order = 2 * nz
    f32, bf16 = jnp.float32, jnp.bfloat16
    vmem = pl.BlockSpec(memory_space=pltpu.VMEM)
    hbm = pl.BlockSpec(memory_space=pltpu.HBM)
    plane_x = jax.ShapeDtypeStruct((ny, nz), f32)
    plane_y = jax.ShapeDtypeStruct((nx, nz), f32)
    planes = (plane_y, plane_x, plane_x, plane_y)
    field = jax.ShapeDtypeStruct((nx * ny, nz), f32)
    edge_columns = 2 * (nx + ny)

    def call(kernel, name, columns, limit=16, **options):
        return pl.pallas_call(
            lambda *refs: kernel(nx, ny, *refs),
            compiler_params=pltpu.CompilerParams(vmem_limit_bytes=limit * MIB),
            cost_estimate=pl.CostEstimate(
                flops=6 * columns * order * order,
                bytes_accessed=columns * nz * 4,
                transcendentals=0,
            ),
            name=name,
            **options,
        )

    def swapped(sends):
        return tuple(paired(block, *route) for block, route in zip(sends, ROUTES))

    *sends, coef_edges = call(
        first_edges_kernel,
        "first_edges",
        edge_columns,
        in_specs=[hbm] * 4,
        out_specs=[vmem] * 5,
        out_shape=planes + (jax.ShapeDtypeStruct((edge_columns, nz), f32),),
        scratch_shapes=[
            pltpu.VMEM((2, ny, nz), f32),
            pltpu.VMEM((2, nx, nz), f32),
            pltpu.VMEM((2, ny, nz), bf16),
            pltpu.VMEM((2, nx, TILE, nz), bf16),
            pltpu.VMEM((ny, nz), f32),
            pltpu.VMEM((nx, nz), f32),
            pltpu.SemaphoreType.DMA((10,)),
        ],
    )(
        *(
            pltpu.with_memory_space_constraint(array, pltpu.HBM)
            for array in (theta_pert, sound_coef, flux_east, flux_north)
        )
    )
    arrays = (flux_east, flux_north, flux_up, theta_pert, density, sound_coef)
    flat = tuple(array.reshape(nx * ny, nz) for array in arrays)
    sends, flat, vert_inverse = lax.optimization_barrier((sends, flat, vert_inverse))
    u, v, w, th, rho, coef = flat
    halo = swapped(sends)
    h, g, mat, u, v, th, coef = call(
        prepare_kernel,
        "prepare",
        nx * ny,
        in_specs=[hbm] * 5,
        out_specs=[vmem] * 7,
        out_shape=(field, field, jax.ShapeDtypeStruct((3 * order, order), bf16))
        + (field,) * 3
        + (jax.ShapeDtypeStruct((nx * ny, nz), bf16),),
        scratch_shapes=[pltpu.VMEM((order, order), f32), pltpu.SemaphoreType.DMA((5,))],
    )(*(pltpu.with_memory_space_constraint(x, pltpu.HBM) for x in (vert_inverse, u, v, th, coef)))
    edge_state = tuple(array.reshape(nx, ny, nz) for array in (h, w, th, g))
    for substep in range(SUBSTEPS - 1):
        new_state = call(
            functools.partial(edges_kernel, substep > 0),
            "edges",
            edge_columns,
            in_specs=[vmem] * 11,
            out_specs=[vmem] * 8,
            out_shape=planes + (jax.ShapeDtypeStruct((edge_columns, nz), f32),) * 4,
        )(mat, coef_edges, *edge_state, g.reshape(nx, ny, nz), *halo)
        sends, edge_state = new_state[:4], new_state[4:]
        arrived = swapped(sends)
        g, h, w, th, u, v, rho = call(
            block_kernel,
            "block",
            nx * ny,
            in_specs=[vmem] * 17,
            out_specs=[vmem] * 7,
            out_shape=(field,) * 7,
        )(mat, coef, g, h, w, th, u, v, rho, *edge_state, *halo)
        halo = arrived
    outs = call(
        last_kernel,
        "last",
        nx * ny,
        limit=24,
        in_specs=[vmem] * 12,
        out_specs=[hbm] * 5,
        out_shape=(field,) * 5,
        scratch_shapes=[pltpu.VMEM((nx * ny, nz), f32)] * 5
        + [
            pltpu.SemaphoreType.DMA((3 * (nx // LAST_ROWS),)),
            pltpu.SemaphoreType.DMA((2 * (nx // FLUX_ROWS),)),
        ],
    )(mat, g, h, w, th, u, v, rho, *halo)
    return tuple(out.reshape(nx, ny, nz) for out in outs)


def solution(mesh):
    spec = P("gx", "gy", None)
    return jax.shard_map(
        body, mesh=mesh, in_specs=(spec,) * 6 + (P(),), out_specs=(spec,) * 5, check_vma=False
    )
```
